128 devices in a mesh: tau: 8 (over x, core), tile: 16 (over z, y).
Axes of the slice: x: 4, y: 4, z: 4, core: 2. Of those that a mesh axis runs over, the one named last changes fastest.
Arguments:
- occupied: bfloat16 [8, 2048, 128, 128], P('tau', 'tile'), may hold values from -6 to 6
- virtual: bfloat16 [8, 2048, 128, 128], P('tau', 'tile'), may hold values from -0.125 to 0.125
- cos_weights: float32 [4, 8], replicated, may hold values from -1 to 1
- pair_occ: int32 [3072, 16], P('tile'), may hold values from 0 to 127
- pair_virt: int32 [3072, 16], P('tile'), may hold values from 0 to 127
- partial_target_tile: int32 [3072], P('tile'), may hold values from 0 to 511, as said below
Outputs:
- spectrum: float32 [4, 512, 128, 128], P(None, 'tile', 'tau')
The draws below stay inside these ranges and needn't reach their ends.
Inputs may be any that keep to these rules, and one draw needn't show every extreme that they name: `partial_target_tile`: within each aligned block of 192 entries, no owner (values d * 32 to (d + 1) * 32 - 1 for owner d) is named more than 24 times; one owner is named exactly 24 times in every block.
All inputs are finite; a program needn't handle non-finite values.
Results may differ from the reference program's by a relative error of at most 0.0003.
Values sent between devices are 32-bit elements; how exact they have to be, the bound alone decides.
A program may use at most 192 MiB of HBM per device.

```python
import math
import jax
import jax.numpy as jnp
from jax import lax

TILE = 128
TERMS = 16
NFREQ = 4
SLOT_DEV = 128
PART_DEV = 192
CHI_DEV = 32
NTAU = 8
NOCC = 2048
NPART = 3072
NCHI = 512
CAP = 24


def draw_partial_target_tile(key, part):
    owners = NPART // PART_DEV
    first, second, third, fourth = jax.random.split(jax.random.fold_in(key, 7), 4)
    complete_holder = jax.random.randint(first, (), 0, owners)
    owner_preference = jax.random.randint(second, (owners, owners), 0, 1 << 19)
    random_perturbation = jax.random.randint(third, (owners, owners, CAP), 0, 1 << 19)
    holder_indices = jnp.arange(owners, dtype=jnp.int32)
    extra_credit = jnp.where(holder_indices == complete_holder, 1 << 20, 0).astype(jnp.int32)
    ranking_value = owner_preference[:, :, None] + random_perturbation + extra_credit[None, :, None]
    places = jnp.arange(owners * CAP, dtype=jnp.int32).reshape(owners, CAP)
    ranking_value = ranking_value * (owners * CAP) + places[None]
    flat = ranking_value.reshape(owners, owners * CAP)
    _, chosen = lax.top_k(flat, PART_DEV)
    owner = (chosen // CAP).astype(jnp.int32)
    within = jax.random.randint(fourth, (owners, PART_DEV), 0, CHI_DEV)
    return (owner * CHI_DEV + within).reshape(-1).astype(jnp.int32)


def touch_ends(drawn, stream_key, low, largest):
    longest = drawn.shape.index(max(drawn.shape))
    spots = []
    for shift in (0, 1):
        where = [jax.random.randint(jax.random.fold_in(stream_key, axis), (), 0, length) for axis, length in enumerate(drawn.shape)]
        where[longest] = (where[longest] + shift) % drawn.shape[longest]
        spots.append(tuple(where))
    return drawn.at[spots[0]].set(low).at[spots[1]].set(largest)


def level_of(rng, dims, pieces, least, largest):
    factor_of = 1.0
    for position, parts in pieces:
        draws = jax.random.uniform(jax.random.fold_in(jax.random.fold_in(rng, 6), position), (parts,), jnp.float32, least / len(pieces), largest / len(pieces))
        factor_of = factor_of * jnp.repeat(jnp.exp(draws), dims[position] // parts).reshape((-1,) + (1,) * (len(dims) - 1 - position))
    return factor_of


def noise(rng, dims, width, reach, cuts=(), held_as=jnp.bfloat16):
    array = width * jax.random.normal(rng, dims, jnp.float32)
    if cuts:
        array = array * level_of(rng, dims, cuts, -0.22, 0.18)
    return jnp.clip(array, -reach, reach).astype(held_as)


def setup_inputs(seed: int = 0) -> dict:
    splits = jax.random.split(jax.random.key(seed), 7)
    return {
        "occupied": noise(splits[0], (NTAU, NOCC, TILE, TILE), 1.0, 6.0, ((0, 8), (1, 16))),
        "virtual": noise(splits[1], (NTAU, NOCC, TILE, TILE), (TILE * TERMS) ** -0.5, 0.125, ((0, 8), (1, 16))),
        "cos_weights": jnp.clip(jax.random.uniform(splits[2], (NFREQ, NTAU), jnp.float32, -1.0, 1.0), -1.0, 1.0),
        "pair_occ": touch_ends(jax.random.randint(splits[3], (NPART, TERMS), 0, SLOT_DEV), jax.random.fold_in(splits[3], 1), 0, SLOT_DEV - 1).astype(jnp.int32),
        "pair_virt": touch_ends(jax.random.randint(splits[4], (NPART, TERMS), 0, SLOT_DEV), jax.random.fold_in(splits[4], 1), 0, SLOT_DEV - 1).astype(jnp.int32),
        "partial_target_tile": draw_partial_target_tile(jax.random.fold_in(splits[6], 71), 0),
    }


def reference(occupied, virtual, cos_weights, pair_occ, pair_virt, partial_target_tile):
    owner_base = (jnp.arange(NPART, dtype=jnp.int32) // PART_DEV) * SLOT_DEV
    occ_global = (pair_occ + owner_base[:, None]).astype(jnp.int32)
    virt_global = (pair_virt + owner_base[:, None]).astype(jnp.int32)
    group = math.gcd(NPART, 16)
    count = NPART // group
    occ_blocks = occ_global.reshape(count, group, TERMS)
    virt_blocks = virt_global.reshape(count, group, TERMS)
    dest_blocks = partial_target_tile.astype(jnp.int32).reshape(count, group)

    def time_step(spectrum, step_index):
        occ_now = lax.dynamic_index_in_dim(occupied, step_index, 0, keepdims=False)
        virt_now = lax.dynamic_index_in_dim(virtual, step_index, 0, keepdims=False)

        def add_block(chi_time, items):
            left = jnp.take(occ_now, items[0], axis=0).astype(jnp.float32)
            right = jnp.take(virt_now, items[1], axis=0).astype(jnp.float32)
            product = jnp.einsum("bjrk,bjkc->brc", left, right, precision=lax.Precision.HIGHEST)
            return chi_time.at[items[2]].add(product), None

        chi_time, _ = lax.scan(add_block, jnp.zeros((NCHI, TILE, TILE), jnp.float32),
                               (occ_blocks, virt_blocks, dest_blocks))
        weights = lax.dynamic_index_in_dim(cos_weights, step_index, 1, keepdims=False)
        return spectrum + weights[:, None, None, None] * chi_time[None], None

    spectrum, _ = lax.scan(time_step, jnp.zeros((NFREQ, NCHI, TILE, TILE), jnp.float32),
                           jnp.arange(NTAU, dtype=jnp.int32))
    return spectrum
```

```python
import functools

import jax
import jax.numpy as jnp
from jax import lax
from jax.experimental import pallas as pl
from jax.experimental.pallas import tpu as pltpu
from jax.sharding import PartitionSpec as P

CHI_DEV = 32
MESH = pl.DeviceIdType.MESH


def chunks_of(cap):
    return 8 if cap % 8 == 0 else 2


def tables(target, chi_dev, owners, cap, chunks):
    parts = target.shape[0]
    deep = cap // chunks
    index = jnp.arange(parts, dtype=jnp.int32)
    owner = target // chi_dev
    key = owner * parts + index
    position = jnp.sum((key[None, :] < key[:, None]).astype(jnp.int32), axis=1)
    hit = position[:, None] == index[None, :]
    order = jnp.sum(jnp.where(hit, index[:, None], 0), axis=0)
    names = jnp.arange(owners, dtype=jnp.int32)
    first = jnp.sum((owner[:, None] < names[None, :]).astype(jnp.int32), axis=0)
    last = jnp.sum((owner[:, None] <= names[None, :]).astype(jnp.int32), axis=0)
    q = jnp.arange(chunks, dtype=jnp.int32)[:, None, None]
    k = jnp.arange(deep, dtype=jnp.int32)[None, None, :]
    place = first[None, :, None] + (q - first[None, :, None]) % chunks + chunks * k
    filled = place < last[None, :, None]
    source = jnp.minimum(place // chunks, parts // chunks - 1)
    flat = place.reshape(-1)
    local = jnp.sum(jnp.where(position[:, None] == flat[None, :], (target % chi_dev)[:, None], 0), axis=0)
    slot_ids = jnp.where(filled.reshape(-1), local, -1).astype(jnp.float32)
    slot_ids = slot_ids.reshape(chunks, owners, deep).transpose(1, 0, 2).reshape(owners, 1, cap)
    slot_ids = jnp.broadcast_to(jnp.pad(slot_ids, ((0, 0), (0, 0), (0, 128 - cap))), (owners, 8, 128))
    return order, source.reshape(-1), slot_ids


def kernel(
    cfg, order, pair_occ, pair_virt, source, weights, occ, virt, ids, out,
    stage, xrecv, spec, ysend, yrecv, idrecv, idwide,
    xs, xr, ys, yr, ids_s, ids_r,
):
    T, B, Q, NB, LX, LY, terms = cfg
    n = stage.shape[2]
    rows, cols = stage.shape[3:]
    freqs, chi = out.shape[:2]
    deep = yrecv.shape[2]
    blocks = yrecv.shape[3]
    t = lax.axis_index("tau")
    b = lax.axis_index("tile")

    barrier = pltpu.get_barrier_semaphore()
    for d in range(1, T):
        pl.semaphore_signal(barrier, inc=1, device_id=(lax.rem(t + d, T), b), device_id_type=MESH)
    for d in range(1, B):
        pl.semaphore_signal(barrier, inc=1, device_id=(t, lax.rem(b + d, B)), device_id_type=MESH)

    def compute(s):
        buf = lax.rem(s, NB)

        def one(i, carry):
            p = order[s + Q * i] * terms
            left = jnp.concatenate([occ[pair_occ[p + j]] for j in range(terms)], axis=1)
            right = jnp.concatenate([virt[pair_virt[p + j]] for j in range(terms)], axis=0)
            product = jnp.dot(left, right, preferred_element_type=jnp.float32)
            for g in range(T):
                stage[buf, g, i] = product[g * rows : (g + 1) * rows]
            return carry

        lax.fori_loop(0, n, one, 0)

    def x_copy(s, d):
        buf = lax.rem(s, NB)
        to = lax.rem(t + d, T)
        return pltpu.make_async_remote_copy(
            src_ref=stage.at[buf, to],
            dst_ref=xrecv.at[s, d - 1],
            send_sem=xs.at[buf],
            recv_sem=xr.at[s],
            device_id=(to, b),
            device_id_type=MESH,
        )

    def x_all(s):
        return pltpu.make_async_remote_copy(
            src_ref=stage.at[lax.rem(s, NB), pl.ds(0, T - 1)],
            dst_ref=xrecv.at[s],
            send_sem=xs.at[lax.rem(s, NB)],
            recv_sem=xr.at[s],
            device_id=(lax.rem(t + 1, T), b),
            device_id_type=MESH,
        )

    def y_copy(q, d):
        buf = lax.rem(q, NB)
        return pltpu.make_async_remote_copy(
            src_ref=ysend.at[buf, d - 1],
            dst_ref=yrecv.at[q, d],
            send_sem=ys.at[buf],
            recv_sem=yr.at[q],
            device_id=(t, lax.rem(b + d, B)),
            device_id_type=MESH,
        )

    def y_all(q):
        return pltpu.make_async_remote_copy(
            src_ref=ysend.at[lax.rem(q, NB)],
            dst_ref=yrecv.at[q, pl.ds(1, B - 1)],
            send_sem=ys.at[lax.rem(q, NB)],
            recv_sem=yr.at[q],
            device_id=(t, lax.rem(b + 1, B)),
            device_id_type=MESH,
        )

    def id_copy(d):
        to = lax.rem(b + d, B)
        return pltpu.make_async_remote_copy(
            src_ref=ids.at[to],
            dst_ref=idrecv.at[d],
            send_sem=ids_s.at[d],
            recv_sem=ids_r.at[d],
            device_id=(t, to),
            device_id_type=MESH,
        )

    def transform(q):
        buf = lax.rem(q, NB)
        w = [[weights[k * T + lax.rem(t + T - d, T)] for k in range(freqs)] for d in range(T)]

        def one(i, carry):
            total = [None] * freqs
            for d in range(T):
                v = stage[buf, t, i] if d == 0 else xrecv[q, d - 1, i]
                for k in range(freqs):
                    term = v * w[d][k]
                    total[k] = term if total[k] is None else total[k] + term
            for k in range(freqs):
                for r in range(rows // 8):
                    spec[i, k * (rows // 8) + r] = total[k][r * 8 : r * 8 + 8]
            return carry

        lax.fori_loop(0, n, one, 0)

    def pack(q):
        buf = lax.rem(q, NB)
        for k in range(deep):
            yrecv[q, 0, k] = spec[source[(q * B + b) * deep + k]]

        def one(d, carry):
            at = (q * B + lax.rem(b + d, B)) * deep
            for k in range(deep):
                ysend[buf, d - 1, k] = spec[source[at + k]]
            return carry

        lax.fori_loop(1, B, one, 0)

    def widen():
        def one(d, carry):
            v = idrecv[d]
            for s in range(Q * deep):
                idwide[s // deep, d, s % deep] = jnp.broadcast_to(v[:, s : s + 1], v.shape)
            return carry

        lax.fori_loop(0, B, one, 0)

    def reduce(q):
        def one(c, carry):
            want = c.astype(jnp.float32)
            total = None
            for d in range(B):
                for k in range(deep):
                    same = idwide[q, d, k] == want
                    part = jnp.where(same[None], yrecv[q, d, k], 0.0)
                    total = part if total is None else total + part
            total = total.reshape(freqs, rows, cols)
            out[:, c] = jnp.where(q > 0, out[:, c], 0.0) + total
            return carry

        lax.fori_loop(0, chi, one, 0)

    def step(s, carry):
        @pl.when(s < Q)
        def _():
            @pl.when(s >= NB)
            def _():
                x_all(s - NB).wait_send()

            compute(s)

            @pl.when(s == 0)
            def _():
                pl.semaphore_wait(barrier, T - 1 + B - 1)
                for d in range(1, B):
                    id_copy(d).start()

            for d in range(1, T):
                x_copy(s, d).start()

        @pl.when(s == LX)
        def _():
            idrecv[0] = ids[b]
            for d in range(1, B):
                id_copy(d).wait()
            widen()

        @pl.when(jnp.logical_and(s >= LX, s < Q + LX))
        def _():
            q = s - LX
            x_all(q).wait_recv()
            transform(q)

            @pl.when(q >= NB)
            def _():
                y_all(q - NB).wait_send()

            pack(q)
            for d in range(1, B):
                y_copy(q, d).start()

        @pl.when(s >= LX + LY)
        def _():
            q = s - LX - LY
            y_all(q).wait_recv()
            reduce(q)

        return carry

    lax.fori_loop(0, Q + LX + LY, step, 0)
    for i in range(min(NB, Q)):
        x_all(Q - 1 - i).wait_send()
        y_all(Q - 1 - i).wait_send()


def body(occupied, virtual, cos_weights, pair_occ, pair_virt, partial_target_tile):
    B = lax.axis_size("tile")
    T = lax.axis_size("tau")
    parts, terms = pair_occ.shape
    cap = 2 * parts // B
    freqs = cos_weights.shape[0]
    slots, size = occupied.shape[1:3]
    rows = size // T
    Q = chunks_of(cap)
    NB, LX, LY = min(4, Q), 2, 2
    n, deep, blocks = parts // Q, cap // Q, freqs * rows // 8
    order, source, ids = tables(partial_target_tile, CHI_DEV, B, cap, Q)
    f32 = jnp.float32
    smem = pl.BlockSpec(memory_space=pltpu.SMEM)
    vmem = pl.BlockSpec(memory_space=pltpu.VMEM)
    dma = pltpu.SemaphoreType.DMA
    return pl.pallas_call(
        functools.partial(kernel, (T, B, Q, NB, LX, LY, terms)),
        out_shape=jax.ShapeDtypeStruct((freqs, CHI_DEV, rows, size), f32),
        in_specs=[smem] * 5 + [vmem] * 3,
        out_specs=vmem,
        scratch_shapes=[
            pltpu.VMEM((NB, T, n, rows, size), f32),
            pltpu.VMEM((Q, T - 1, n, rows, size), f32),
            pltpu.VMEM((n, blocks, 8, size), f32),
            pltpu.VMEM((NB, B - 1, deep, blocks, 8, size), f32),
            pltpu.VMEM((Q, B, deep, blocks, 8, size), f32),
            pltpu.VMEM((B, 8, 128), f32),
            pltpu.VMEM((Q, B, deep, 8, 128), f32),
            dma((NB,)),
            dma((Q,)),
            dma((NB,)),
            dma((Q,)),
            dma((B,)),
            dma((B,)),
        ],
        compiler_params=pltpu.CompilerParams(
            collective_id=0, has_side_effects=True, vmem_limit_bytes=62 * 1024 * 1024
        ),
        name="products",
    )(
        order,
        pair_occ.reshape(-1),
        pair_virt.reshape(-1),
        source,
        cos_weights.reshape(-1),
        occupied.reshape(slots, size, size),
        virtual.reshape(slots, size, size),
        ids,
    )


def solution(mesh):
    in_specs = (
        P("tau", "tile", None, None),
        P("tau", "tile", None, None),
        P(),
        P("tile", None),
        P("tile", None),
        P("tile"),
    )
    out_specs = P(None, "tile", "tau", None)
    return jax.shard_map(body, mesh=mesh, in_specs=in_specs, out_specs=out_specs, check_vma=False)
```

```python
import functools
import math

import jax
import jax.numpy as jnp
from jax import lax
from jax.experimental import pallas as pl
from jax.experimental.pallas import tpu as pltpu
from jax.sharding import PartitionSpec as P

CHI_DEV = 32
MESH = pl.DeviceIdType.MESH


def chunks_of(cap):
    return 24 if cap % 24 == 0 else cap


def tables(target_ref, padded, table, idrow, Q, owners, chi_dev):
    i32 = jnp.int32
    N, M = target_ref.shape[1], padded.shape[1]
    S = Q * owners
    padded[...] = jnp.full(padded.shape, owners * chi_dev, i32)
    padded[:, pl.ds(0, N)] = target_ref[...]
    target = padded[...]
    up = lax.broadcasted_iota(i32, (M, M), 0)
    across = lax.broadcasted_iota(i32, (M, M), 1)

    def column(row):
        return jnp.transpose(jnp.broadcast_to(row, (8, M)))[:, 0:1]

    def total(chosen, value):
        return jnp.sum(jnp.where(chosen, value, 0), axis=0, keepdims=True)

    key = (target // chi_dev) * M + lax.broadcasted_iota(i32, (1, M), 1)
    target_col = column(target)
    own_col, local_col = target_col // chi_dev, target_col % chi_dev
    key_col = own_col * M + lax.broadcasted_iota(i32, (M, 1), 0)
    place_col = column(total(key_col < key, jnp.ones((M, M), i32)))
    order = total(place_col == across, up)
    slot = lax.broadcasted_iota(i32, (1, S), 1)
    name = slot % owners
    chunk = slot // owners
    one = jnp.ones((M, S), i32)
    first = total(own_col < name, one)
    last = total(own_col <= name, one)
    offset = chunk - first % Q
    place = first + jnp.where(offset < 0, offset + Q, offset)
    found = total(place_col == place, jnp.broadcast_to(local_col, (M, S)))
    idrow[...] = jnp.where(place < last, found, -1).astype(jnp.float32)
    table[pl.ds(0, 1), pl.ds(0, M)] = jnp.minimum(order, N - 1)
    table[pl.ds(1, 1), pl.ds(0, S)] = jnp.minimum(place // Q, N // Q - 1)


def around(me, offset, sizes):
    (a, b), (big, small) = offset, sizes
    return lax.rem(me // small + a, big) * small + lax.rem(me + b, small)


def offsets(sizes):
    every = [(a, b) for a in range(sizes[0]) for b in range(sizes[1])]
    far = lambda v, n: min(v, n - v)
    return sorted(every, key=lambda o: (far(o[0], sizes[0]) + far(o[1], sizes[1]), o[0] * o[1] > 0, o[0] + o[1], o))


def back(offset, sizes):
    return tuple((n - v) % n for v, n in zip(offset, sizes))


def kernel(
    cfg, pair_occ, pair_virt, weights, target, occ_hbm, virt_hbm, out,
    occ, virt, stage, xrecv, spec, ysend, yrecv, padded, table, smem, idrow, idrecv, idwide,
    xs, xr, ys, yr, ids_s, ids_r, load,
):
    tau, tile, Q, NB, LX, LY = cfg
    T, B = tau[0] * tau[1], tile[0] * tile[1]
    terms = pair_occ.shape[0]
    n = stage.shape[2]
    rows, cols = stage.shape[3:]
    freqs, chi = out.shape[:2]
    t = lax.axis_index("tau")
    b = lax.axis_index("tile")
    near_t, near_b = offsets(tau), offsets(tile)

    def tau_at(d):
        return around(t, near_t[d], tau)

    def tile_at(d):
        return around(b, near_b[d], tile)

    loads = [
        pltpu.make_async_copy(occ_hbm, occ, load.at[0]),
        pltpu.make_async_copy(virt_hbm, virt, load.at[1]),
    ]
    for copy in loads:
        copy.start()
    barrier = pltpu.get_barrier_semaphore()
    for d in range(1, T):
        pl.semaphore_signal(barrier, inc=1, device_id=(tau_at(d), b), device_id_type=MESH)
    for d in range(1, B):
        pl.semaphore_signal(barrier, inc=1, device_id=(t, tile_at(d)), device_id_type=MESH)
    tables(target, padded, table, idrow, Q, B, chi)
    down = pltpu.make_async_copy(table, smem, load.at[2])
    down.start()
    down.wait()
    for copy in loads:
        copy.wait()

    def compute(s):
        buf = lax.rem(s, NB)

        def one(i, carry):
            p = smem[0, s + Q * i]
            left = jnp.concatenate([occ[pair_occ[j, p]] for j in range(terms)], axis=1)
            right = jnp.concatenate([virt[pair_virt[j, p]] for j in range(terms)], axis=0)
            product = jnp.dot(left, right, preferred_element_type=jnp.float32)
            for g in range(T):
                stage[buf, g, i] = product[g * rows : (g + 1) * rows]
            return carry

        lax.fori_loop(0, n, one, 0)

    def x_copy(s, d):
        buf = lax.rem(s, NB)
        to = tau_at(d)
        return pltpu.make_async_remote_copy(
            src_ref=stage.at[buf, to],
            dst_ref=xrecv.at[s, d - 1],
            send_sem=xs.at[buf],
            recv_sem=xr.at[s],
            device_id=(to, b),
            device_id_type=MESH,
        )

    def x_all(s):
        return pltpu.make_async_remote_copy(
            src_ref=stage.at[lax.rem(s, NB), pl.ds(0, T - 1)],
            dst_ref=xrecv.at[s],
            send_sem=xs.at[lax.rem(s, NB)],
            recv_sem=xr.at[s],
            device_id=(tau_at(1), b),
            device_id_type=MESH,
        )

    def y_copy(q, d):
        buf = lax.rem(q, NB)
        return pltpu.make_async_remote_copy(
            src_ref=ysend.at[buf, d - 1],
            dst_ref=yrecv.at[q, d],
            send_sem=ys.at[buf],
            recv_sem=yr.at[q],
            device_id=(t, tile_at(d)),
            device_id_type=MESH,
        )

    def y_all(q):
        return pltpu.make_async_remote_copy(
            src_ref=ysend.at[lax.rem(q, NB)],
            dst_ref=yrecv.at[q, pl.ds(1, B - 1)],
            send_sem=ys.at[lax.rem(q, NB)],
            recv_sem=yr.at[q],
            device_id=(t, tile_at(1)),
            device_id_type=MESH,
        )

    def id_copy(d):
        return pltpu.make_async_remote_copy(
            src_ref=idrow,
            dst_ref=idrecv.at[d],
            send_sem=ids_s.at[d],
            recv_sem=ids_r.at[d],
            device_id=(t, tile_at(d)),
            device_id_type=MESH,
        )

    def transform(q):
        buf = lax.rem(q, NB)
        w = [[weights[k, around(t, back(near_t[d], tau), tau)] for k in range(freqs)] for d in range(T)]

        def one(i, carry):
            total = [None] * freqs
            for d in range(T):
                v = stage[buf, t, i] if d == 0 else xrecv[q, d - 1, i]
                for k in range(freqs):
                    term = v * w[d][k]
                    total[k] = term if total[k] is None else total[k] + term
            for k in range(freqs):
                for r in range(rows // 8):
                    spec[i, k * (rows // 8) + r] = total[k][r * 8 : r * 8 + 8]
            return carry

        lax.fori_loop(0, n, one, 0)

    def pack(q):
        buf = lax.rem(q, NB)
        yrecv[q, 0] = spec[smem[1, q * B + b]]
        for d in range(1, B):
            ysend[buf, d - 1] = spec[smem[1, q * B + tile_at(d)]]
            y_copy(q, d).start()

    def widen():
        S = Q * B
        ids = jnp.concatenate([idrecv[d] for d in range(B)], axis=0).astype(jnp.bfloat16)
        slot = lax.broadcasted_iota(jnp.int32, (S, cols), 0)

        def one(q, carry):
            pick = jnp.where(slot == q * B + b, 1.0, 0.0).astype(jnp.bfloat16)
            idwide[q] = jnp.dot(ids, pick, preferred_element_type=jnp.float32)
            return carry

        lax.fori_loop(0, Q, one, 0)

    def reduce(q):
        def one(c, carry):
            want = c.astype(jnp.float32)
            total = None
            for d in range(B):
                same = jnp.broadcast_to(idwide[q, pl.ds(d, 1)], (8, cols)) == want
                part = jnp.where(same[None], yrecv[q, d], 0.0)
                total = part if total is None else total + part
            total = total.reshape(freqs, rows, cols)
            out[:, c] = jnp.where(q > 0, out[:, c], 0.0) + total
            return carry

        lax.fori_loop(0, chi, one, 0)

    def step(s, carry):
        @pl.when(s < Q)
        def _():
            @pl.when(s >= NB)
            def _():
                x_all(s - NB).wait_send()

            compute(s)

            @pl.when(s == 0)
            def _():
                pl.semaphore_wait(barrier, T - 1 + B - 1)
                for d in range(1, B):
                    id_copy(d).start()

            for d in range(1, T):
                x_copy(s, d).start()

        @pl.when(s == LX)
        def _():
            idrecv[0] = idrow[...]
            for d in range(1, B):
                id_copy(d).wait()
            widen()

        @pl.when(jnp.logical_and(s >= LX, s < Q + LX))
        def _():
            q = s - LX
            x_all(q).wait_recv()
            transform(q)

            @pl.when(q >= NB)
            def _():
                y_all(q - NB).wait_send()

            pack(q)

        @pl.when(s >= LX + LY)
        def _():
            q = s - LX - LY
            y_all(q).wait_recv()
            reduce(q)

        return carry

    lax.fori_loop(0, Q + LX + LY, step, 0)
    for i in range(min(NB, Q)):
        x_all(Q - 1 - i).wait_send()
        y_all(Q - 1 - i).wait_send()


def pair_of(size, small):
    return (size // small, small)


def body(occupied, virtual, cos_weights, pair_occ, pair_virt, partial_target_tile):
    B = lax.axis_size("tile")
    T = lax.axis_size("tau")
    parts, terms = pair_occ.shape
    freqs = cos_weights.shape[0]
    slots, size = occupied.shape[1:3]
    rows = size // T
    Q = chunks_of(2 * parts // B)
    NB, LX, LY = min(6, Q), 3, 3
    n, blocks = parts // Q, freqs * rows // 8
    f32 = jnp.float32
    smem = pl.BlockSpec(memory_space=pltpu.SMEM)
    vmem = pl.BlockSpec(memory_space=pltpu.VMEM)
    hbm = pl.BlockSpec(memory_space=pl.ANY)
    dma = pltpu.SemaphoreType.DMA
    full = -(-parts // 128) * 128
    wide = max(full, Q * B)
    return pl.pallas_call(
        functools.partial(kernel, (pair_of(T, 2), pair_of(B, math.isqrt(B)), Q, NB, LX, LY)),
        out_shape=jax.ShapeDtypeStruct((freqs, CHI_DEV, rows, size), f32),
        in_specs=[smem] * 3 + [vmem, hbm, hbm],
        out_specs=vmem,
        scratch_shapes=[
            pltpu.VMEM((slots, size, size), occupied.dtype),
            pltpu.VMEM((slots, size, size), virtual.dtype),
            pltpu.VMEM((NB, T, n, rows, size), f32),
            pltpu.VMEM((Q, T - 1, n, rows, size), f32),
            pltpu.VMEM((n, blocks, 8, size), f32),
            pltpu.VMEM((NB, B - 1, blocks, 8, size), f32),
            pltpu.VMEM((Q, B, blocks, 8, size), f32),
            pltpu.VMEM((1, full), jnp.int32),
            pltpu.VMEM((8, wide), jnp.int32),
            pltpu.SMEM((8, wide), jnp.int32),
            pltpu.VMEM((1, Q * B), f32),
            pltpu.VMEM((B, 1, Q * B), f32),
            pltpu.VMEM((Q, B, size), f32),
            dma((NB,)),
            dma((Q,)),
            dma((NB,)),
            dma((Q,)),
            dma((B,)),
            dma((B,)),
            dma((3,)),
        ],
        compiler_params=pltpu.CompilerParams(
            collective_id=0, has_side_effects=True, vmem_limit_bytes=60 * 1024 * 1024
        ),
        name="products",
    )(
        pair_occ.T,
        pair_virt.T,
        cos_weights,
        partial_target_tile.reshape(1, parts),
        occupied.reshape(slots, size, size),
        virtual.reshape(slots, size, size),
    )


def solution(mesh):
    in_specs = (
        P("tau", "tile", None, None),
        P("tau", "tile", None, None),
        P(),
        P("tile", None),
        P("tile", None),
        P("tile"),
    )
    out_specs = P(None, "tile", "tau", None)
    return jax.shard_map(body, mesh=mesh, in_specs=in_specs, out_specs=out_specs, check_vma=False)
```

```python
import functools
import math

import jax
import jax.numpy as jnp
from jax import lax
from jax.experimental import pallas as pl
from jax.experimental.pallas import tpu as pltpu
from jax.sharding import PartitionSpec as P

CHI_DEV = 32
UNROLL = 2
MESH = pl.DeviceIdType.MESH


def chunks_of(cap):
    return 24 if cap % 24 == 0 else cap


def tables(target_ref, padded, table, idrow, Q, owners, chi_dev):
    i32 = jnp.int32
    N, M = target_ref.shape[1], padded.shape[1]
    S = Q * owners
    padded[...] = jnp.full(padded.shape, owners * chi_dev, i32)
    padded[:, pl.ds(0, N)] = target_ref[...]
    target = padded[...]
    up = lax.broadcasted_iota(i32, (M, M), 0)
    across = lax.broadcasted_iota(i32, (M, M), 1)

    def column(row):
        return jnp.transpose(jnp.broadcast_to(row, (8, M)))[:, 0:1]

    def total(chosen, value):
        return jnp.sum(jnp.where(chosen, value, 0), axis=0, keepdims=True)

    key = (target // chi_dev) * M + lax.broadcasted_iota(i32, (1, M), 1)
    target_col = column(target)
    own_col, local_col = target_col // chi_dev, target_col % chi_dev
    key_col = own_col * M + lax.broadcasted_iota(i32, (M, 1), 0)
    place_col = column(total(key_col < key, jnp.ones((M, M), i32)))
    order = total(place_col == across, up)
    slot = lax.broadcasted_iota(i32, (1, S), 1)
    name = slot % owners
    chunk = slot // owners
    one = jnp.ones((M, S), i32)
    first = total(own_col < name, one)
    last = total(own_col <= name, one)
    offset = chunk - first % Q
    place = first + jnp.where(offset < 0, offset + Q, offset)
    found = total(place_col == place, jnp.broadcast_to(local_col, (M, S)))
    idrow[...] = jnp.where(place < last, found, -1).astype(jnp.float32)
    table[pl.ds(0, 1), pl.ds(0, M)] = jnp.minimum(order, N - 1)
    table[pl.ds(1, 1), pl.ds(0, S)] = jnp.minimum(place // Q, N // Q - 1)


def around(me, offset, sizes):
    (a, b), (big, small) = offset, sizes
    return lax.rem(me // small + a, big) * small + lax.rem(me + b, small)


def offsets(sizes):
    every = [(a, b) for a in range(sizes[0]) for b in range(sizes[1])]
    far = lambda v, n: min(v, n - v)
    return every[:1] + sorted(every[1:], reverse=True, key=lambda o: (far(o[0], sizes[0]) + far(o[1], sizes[1]), o[0] * o[1] > 0, o[0] + o[1], o))


def back(offset, sizes):
    return tuple((n - v) % n for v, n in zip(offset, sizes))


def kernel(
    cfg, pair_occ_hbm, pair_virt_hbm, weights, target_hbm, occ_hbm, virt_hbm, out,
    pair_occ, pair_virt, target, occ, virt, stage, xrecv, spec, ysend, yrecv, padded, table, smem, idrow, idrecv, idwide,
    xs, xr, ys, yr, ids_s, ids_r, load,
):
    tau, tile, Q, NB, LX, LY = cfg
    T, B = tau[0] * tau[1], tile[0] * tile[1]
    terms = pair_occ.shape[0]
    n = stage.shape[2]
    rows, cols = stage.shape[3:]
    freqs, chi = out.shape[:2]
    t = lax.axis_index("tau")
    b = lax.axis_index("tile")
    near_t, near_b = offsets(tau), offsets(tile)

    def tau_at(d):
        return around(t, near_t[d], tau)

    def tile_at(d):
        return around(b, near_b[d], tile)

    names = pltpu.make_async_copy(target_hbm, target, load.at[3])
    names.start()
    loads = [
        pltpu.make_async_copy(pair_occ_hbm, pair_occ, load.at[4]),
        pltpu.make_async_copy(pair_virt_hbm, pair_virt, load.at[5]),
        pltpu.make_async_copy(occ_hbm, occ, load.at[0]),
        pltpu.make_async_copy(virt_hbm, virt, load.at[1]),
    ]
    for copy in loads:
        copy.start()
    barrier = pltpu.get_barrier_semaphore()
    for d in range(1, T):
        pl.semaphore_signal(barrier, inc=1, device_id=(tau_at(d), b), device_id_type=MESH)
    for d in range(1, B):
        pl.semaphore_signal(barrier, inc=1, device_id=(t, tile_at(d)), device_id_type=MESH)
    names.wait()
    tables(target, padded, table, idrow, Q, B, chi)
    down = pltpu.make_async_copy(table, smem, load.at[2])
    down.start()
    down.wait()
    for copy in loads:
        copy.wait()

    def compute(s, lo, hi):
        buf = lax.rem(s, NB)

        def some(step, carry):
            for u in range(UNROLL):
                i = step * UNROLL + u
                p = smem[0, s + Q * i]
                left = jnp.concatenate([occ[pair_occ[j, p]] for j in range(terms)], axis=1)
                right = jnp.concatenate([virt[pair_virt[j, p]] for j in range(terms)], axis=0)
                product = jnp.dot(left, right, preferred_element_type=jnp.float32)
                for g in range(T):
                    stage[buf, g, i] = product[g * rows : (g + 1) * rows]
            return carry

        lax.fori_loop(lo // UNROLL, hi // UNROLL, some, 0)

    def x_copy(s, d, lo, size):
        buf = lax.rem(s, NB)
        to = tau_at(d)
        return pltpu.make_async_remote_copy(
            src_ref=stage.at[buf, to, pl.ds(lo, size)],
            dst_ref=xrecv.at[s, d - 1, pl.ds(lo, size)],
            send_sem=xs.at[buf],
            recv_sem=xr.at[s],
            device_id=(to, b),
            device_id_type=MESH,
        )

    def x_all(s):
        return pltpu.make_async_remote_copy(
            src_ref=stage.at[lax.rem(s, NB), pl.ds(0, T - 1)],
            dst_ref=xrecv.at[s],
            send_sem=xs.at[lax.rem(s, NB)],
            recv_sem=xr.at[s],
            device_id=(tau_at(1), b),
            device_id_type=MESH,
        )

    def y_copy(q, d):
        buf = lax.rem(q, NB)
        return pltpu.make_async_remote_copy(
            src_ref=ysend.at[buf, d - 1],
            dst_ref=yrecv.at[q, d],
            send_sem=ys.at[buf],
            recv_sem=yr.at[q],
            device_id=(t, tile_at(d)),
            device_id_type=MESH,
        )

    def y_all(q):
        return pltpu.make_async_remote_copy(
            src_ref=ysend.at[lax.rem(q, NB)],
            dst_ref=yrecv.at[q, pl.ds(1, B - 1)],
            send_sem=ys.at[lax.rem(q, NB)],
            recv_sem=yr.at[q],
            device_id=(t, tile_at(1)),
            device_id_type=MESH,
        )

    def id_copy(d):
        return pltpu.make_async_remote_copy(
            src_ref=idrow,
            dst_ref=idrecv.at[d],
            send_sem=ids_s.at[d],
            recv_sem=ids_r.at[d],
            device_id=(t, tile_at(d)),
            device_id_type=MESH,
        )

    def transform(q):
        buf = lax.rem(q, NB)
        w = [[weights[k, around(t, back(near_t[d], tau), tau)] for k in range(freqs)] for d in range(T)]

        def one(i, carry):
            total = [None] * freqs
            for d in range(T):
                v = stage[buf, t, i] if d == 0 else xrecv[q, d - 1, i]
                for k in range(freqs):
                    term = v * w[d][k]
                    total[k] = term if total[k] is None else total[k] + term
            for k in range(freqs):
                for r in range(rows // 8):
                    spec[i, k * (rows // 8) + r] = total[k][r * 8 : r * 8 + 8]
            return carry

        lax.fori_loop(0, n, one, 0)

    def pack(q):
        buf = lax.rem(q, NB)
        yrecv[q, 0] = spec[smem[1, q * B + b]]
        for d in range(1, B):
            ysend[buf, d - 1] = spec[smem[1, q * B + tile_at(d)]]
            y_copy(q, d).start()

    def widen():
        S = Q * B
        ids = jnp.concatenate([idrecv[d] for d in range(B)], axis=0).astype(jnp.bfloat16)
        slot = lax.broadcasted_iota(jnp.int32, (S, cols), 0)

        def one(q, carry):
            pick = jnp.where(slot == q * B + b, 1.0, 0.0).astype(jnp.bfloat16)
            idwide[q] = jnp.dot(ids, pick, preferred_element_type=jnp.float32)
            return carry

        lax.fori_loop(0, Q, one, 0)

    def reduce(q):
        def one(c, carry):
            want = c.astype(jnp.float32)
            total = None
            for d in range(B):
                same = jnp.broadcast_to(idwide[q, pl.ds(d, 1)], (8, cols)) == want
                part = jnp.where(same[None], yrecv[q, d], 0.0)
                total = part if total is None else total + part
            total = total.reshape(freqs, rows, cols)
            out[:, c] = jnp.where(q > 0, out[:, c], 0.0) + total
            return carry

        lax.fori_loop(0, chi, one, 0)

    def step(s, carry):
        @pl.when(s < Q)
        def _():
            @pl.when(s >= NB)
            def _():
                x_all(s - NB).wait_send()

            @pl.when(s == 0)
            def _():
                compute(s, 0, n // 2)
                pl.semaphore_wait(barrier, T - 1 + B - 1)
                for d in range(1, T):
                    x_copy(s, d, 0, n // 2).start()
                compute(s, n // 2, n)
                for d in range(1, T):
                    x_copy(s, d, n // 2, n - n // 2).start()
                for d in range(1, B):
                    id_copy(d).start()

            @pl.when(s > 0)
            def _():
                compute(s, 0, n)
                for d in range(1, T):
                    x_copy(s, d, 0, n).start()

        @pl.when(s == LX)
        def _():
            idrecv[0] = idrow[...]
            for d in range(1, B):
                id_copy(d).wait()
            widen()

        @pl.when(jnp.logical_and(s >= LX, s < Q + LX))
        def _():
            q = s - LX
            x_all(q).wait_recv()
            transform(q)

            @pl.when(q >= NB)
            def _():
                y_all(q - NB).wait_send()

            pack(q)

        @pl.when(s >= LX + LY)
        def _():
            q = s - LX - LY
            y_all(q).wait_recv()
            reduce(q)

        return carry

    lax.fori_loop(0, Q + LX + LY, step, 0)
    for i in range(min(NB, Q)):
        x_all(Q - 1 - i).wait_send()
        y_all(Q - 1 - i).wait_send()


def pair_of(size, small):
    return (size // small, small)


def body(occupied, virtual, cos_weights, pair_occ, pair_virt, partial_target_tile):
    B = lax.axis_size("tile")
    T = lax.axis_size("tau")
    parts, terms = pair_occ.shape
    freqs = cos_weights.shape[0]
    slots, size = occupied.shape[1:3]
    rows = size // T
    Q = chunks_of(2 * parts // B)
    NB, LX, LY = min(6, Q), 2, 3
    n, blocks = parts // Q, freqs * rows // 8
    f32 = jnp.float32
    smem = pl.BlockSpec(memory_space=pltpu.SMEM)
    vmem = pl.BlockSpec(memory_space=pltpu.VMEM)
    hbm = pl.BlockSpec(memory_space=pl.ANY)
    dma = pltpu.SemaphoreType.DMA
    full = -(-parts // 128) * 128
    wide = max(full, Q * B)
    return pl.pallas_call(
        functools.partial(kernel, (pair_of(T, 2), pair_of(B, math.isqrt(B)), Q, NB, LX, LY)),
        out_shape=jax.ShapeDtypeStruct((freqs, CHI_DEV, rows, size), f32),
        in_specs=[hbm, hbm, smem, hbm, hbm, hbm],
        out_specs=vmem,
        scratch_shapes=[
            pltpu.SMEM((terms, parts), jnp.int32),
            pltpu.SMEM((terms, parts), jnp.int32),
            pltpu.VMEM((1, parts), jnp.int32),
            pltpu.VMEM((slots, size, size), occupied.dtype),
            pltpu.VMEM((slots, size, size), virtual.dtype),
            pltpu.VMEM((NB, T, n, rows, size), f32),
            pltpu.VMEM((Q, T - 1, n, rows, size), f32),
            pltpu.VMEM((n, blocks, 8, size), f32),
            pltpu.VMEM((NB, B - 1, blocks, 8, size), f32),
            pltpu.VMEM((Q, B, blocks, 8, size), f32),
            pltpu.VMEM((1, full), jnp.int32),
            pltpu.VMEM((8, wide), jnp.int32),
            pltpu.SMEM((8, wide), jnp.int32),
            pltpu.VMEM((1, Q * B), f32),
            pltpu.VMEM((B, 1, Q * B), f32),
            pltpu.VMEM((Q, B, size), f32),
            dma((NB,)),
            dma((Q,)),
            dma((NB,)),
            dma((Q,)),
            dma((B,)),
            dma((B,)),
            dma((6,)),
        ],
        compiler_params=pltpu.CompilerParams(
            collective_id=0, has_side_effects=True, vmem_limit_bytes=60 * 1024 * 1024
        ),
        name="products",
    )(
        pair_occ.T,
        pair_virt.T,
        cos_weights,
        partial_target_tile.reshape(1, parts),
        occupied.reshape(slots, size, size),
        virtual.reshape(slots, size, size),
    )


def solution(mesh):
    in_specs = (
        P("tau", "tile", None, None),
        P("tau", "tile", None, None),
        P(),
        P("tile", None),
        P("tile", None),
        P("tile"),
    )
    out_specs = P(None, "tile", "tau", None)
    return jax.shard_map(body, mesh=mesh, in_specs=in_specs, out_specs=out_specs, check_vma=False)
```

```python
import functools
import math

import jax
import jax.numpy as jnp
from jax import lax
from jax.experimental import pallas as pl
from jax.experimental.pallas import tpu as pltpu
from jax.sharding import PartitionSpec as P

CHI_DEV = 32
UNROLL = 2
PAIR = 2
MESH = pl.DeviceIdType.MESH


def chunks_of(cap):
    return 24 if cap % 24 == 0 else cap


def tables(target_ref, padded, table, idrow, Q, owners, chi_dev):
    i32 = jnp.int32
    N, M = target_ref.shape[1], padded.shape[1]
    S = Q * owners
    padded[...] = jnp.full(padded.shape, owners * chi_dev, i32)
    padded[:, pl.ds(0, N)] = target_ref[...]
    target = padded[...]
    up = lax.broadcasted_iota(i32, (M, M), 0)
    across = lax.broadcasted_iota(i32, (M, M), 1)

    def column(row):
        return jnp.transpose(jnp.broadcast_to(row, (8, M)))[:, 0:1]

    def total(chosen, value):
        return jnp.sum(jnp.where(chosen, value, 0), axis=0, keepdims=True)

    key = (target // chi_dev) * M + lax.broadcasted_iota(i32, (1, M), 1)
    target_col = column(target)
    own_col, local_col = target_col // chi_dev, target_col % chi_dev
    key_col = own_col * M + lax.broadcasted_iota(i32, (M, 1), 0)
    place_col = column(total(key_col < key, jnp.ones((M, M), i32)))
    order = total(place_col == across, up)
    slot = lax.broadcasted_iota(i32, (1, S), 1)
    name = slot % owners
    chunk = slot // owners
    one = jnp.ones((M, S), i32)
    first = total(own_col < name, one)
    last = total(own_col <= name, one)
    offset = chunk - first % Q
    place = first + jnp.where(offset < 0, offset + Q, offset)
    found = total(place_col == place, jnp.broadcast_to(local_col, (M, S)))
    idrow[...] = jnp.where(place < last, found, -1).astype(jnp.float32)
    table[pl.ds(0, 1), pl.ds(0, M)] = jnp.minimum(order, N - 1)
    table[pl.ds(1, 1), pl.ds(0, S)] = jnp.minimum(place // Q, N // Q - 1)


def around(me, offset, sizes):
    (a, b), (big, small) = offset, sizes
    return lax.rem(me // small + a, big) * small + lax.rem(me + b, small)


def offsets(sizes):
    every = [(a, b) for a in range(sizes[0]) for b in range(sizes[1])]
    far = lambda v, n: min(v, n - v)
    return every[:1] + sorted(every[1:], reverse=True, key=lambda o: (far(o[0], sizes[0]) + far(o[1], sizes[1]), o[0] * o[1] > 0, o[0] + o[1], o))


def back(offset, sizes):
    return tuple((n - v) % n for v, n in zip(offset, sizes))


def kernel(
    cfg, pair_occ_hbm, pair_virt_hbm, weights, target_hbm, occ_hbm, virt_hbm, out,
    pair_occ, pair_virt, target, occ, virt, stage, xrecv, spec, ysend, yrecv, padded, table, smem, idrow, idrecv, idwide,
    xs, xr, ys, yr, ids_s, ids_r, load,
):
    tau, tile, Q, NB, LX, LY = cfg
    T, B = tau[0] * tau[1], tile[0] * tile[1]
    terms = pair_occ.shape[0]
    n = stage.shape[2]
    rows, cols = stage.shape[3:]
    freqs, chi = out.shape[:2]
    t = lax.axis_index("tau")
    b = lax.axis_index("tile")
    near_t, near_b = offsets(tau), offsets(tile)

    def tau_at(d):
        return around(t, near_t[d], tau)

    def tile_at(d):
        return around(b, near_b[d], tile)

    names = pltpu.make_async_copy(target_hbm, target, load.at[3])
    names.start()
    loads = [
        pltpu.make_async_copy(pair_occ_hbm, pair_occ, load.at[4]),
        pltpu.make_async_copy(pair_virt_hbm, pair_virt, load.at[5]),
        pltpu.make_async_copy(occ_hbm, occ, load.at[0]),
        pltpu.make_async_copy(virt_hbm, virt, load.at[1]),
    ]
    for copy in loads:
        copy.start()
    barrier = pltpu.get_barrier_semaphore()
    for d in range(1, T):
        pl.semaphore_signal(barrier, inc=1, device_id=(tau_at(d), b), device_id_type=MESH)
    for d in range(1, B):
        pl.semaphore_signal(barrier, inc=1, device_id=(t, tile_at(d)), device_id_type=MESH)
    names.wait()
    tables(target, padded, table, idrow, Q, B, chi)
    down = pltpu.make_async_copy(table, smem, load.at[2])
    down.start()
    down.wait()
    for copy in loads:
        copy.wait()

    def compute(s, lo, hi):
        buf = lax.rem(s, NB)

        def some(step, carry):
            for u in range(UNROLL):
                i = step * UNROLL + u
                p = smem[0, s + Q * i]
                left = jnp.concatenate([occ[pair_occ[j, p]] for j in range(terms)], axis=1)
                right = jnp.concatenate([virt[pair_virt[j, p]] for j in range(terms)], axis=0)
                product = jnp.dot(left, right, preferred_element_type=jnp.float32)
                for g in range(T):
                    stage[buf, g, i] = product[g * rows : (g + 1) * rows]
            return carry

        lax.fori_loop(lo // UNROLL, hi // UNROLL, some, 0)

    def x_copy(s, d, lo, size):
        buf = lax.rem(s, NB)
        to = tau_at(d)
        return pltpu.make_async_remote_copy(
            src_ref=stage.at[buf, to, pl.ds(lo, size)],
            dst_ref=xrecv.at[s, d - 1, pl.ds(lo, size)],
            send_sem=xs.at[buf],
            recv_sem=xr.at[s],
            device_id=(to, b),
            device_id_type=MESH,
        )

    def x_all(s):
        return pltpu.make_async_remote_copy(
            src_ref=stage.at[lax.rem(s, NB), pl.ds(0, T - 1)],
            dst_ref=xrecv.at[s],
            send_sem=xs.at[lax.rem(s, NB)],
            recv_sem=xr.at[s],
            device_id=(tau_at(1), b),
            device_id_type=MESH,
        )

    def y_copy(q, d):
        buf = lax.rem(q, NB)
        return pltpu.make_async_remote_copy(
            src_ref=ysend.at[buf, d - 1],
            dst_ref=yrecv.at[q, d],
            send_sem=ys.at[buf],
            recv_sem=yr.at[q],
            device_id=(t, tile_at(d)),
            device_id_type=MESH,
        )

    def y_all(q):
        return pltpu.make_async_remote_copy(
            src_ref=ysend.at[lax.rem(q, NB)],
            dst_ref=yrecv.at[q, pl.ds(1, B - 1)],
            send_sem=ys.at[lax.rem(q, NB)],
            recv_sem=yr.at[q],
            device_id=(t, tile_at(1)),
            device_id_type=MESH,
        )

    def id_copy(d):
        return pltpu.make_async_remote_copy(
            src_ref=idrow,
            dst_ref=idrecv.at[d],
            send_sem=ids_s.at[d],
            recv_sem=ids_r.at[d],
            device_id=(t, tile_at(d)),
            device_id_type=MESH,
        )

    def transform(q):
        buf = lax.rem(q, NB)
        w = [[weights[k, around(t, back(near_t[d], tau), tau)] for k in range(freqs)] for d in range(T)]

        def one(i, carry):
            total = [None] * freqs
            for d in range(T):
                v = stage[buf, t, i] if d == 0 else xrecv[q, d - 1, i]
                for k in range(freqs):
                    term = v * w[d][k]
                    total[k] = term if total[k] is None else total[k] + term
            for k in range(freqs):
                for r in range(rows // 8):
                    spec[i, k * (rows // 8) + r] = total[k][r * 8 : r * 8 + 8]
            return carry

        lax.fori_loop(0, n, one, 0)

    def pack(q):
        buf = lax.rem(q, NB)
        yrecv[q, 0] = spec[smem[1, q * B + b]]
        for d in range(1, B):
            ysend[buf, d - 1] = spec[smem[1, q * B + tile_at(d)]]
            y_copy(q, d).start()

    def widen():
        S = Q * B
        ids = jnp.concatenate([idrecv[d] for d in range(B)], axis=0).astype(jnp.bfloat16)
        slot = lax.broadcasted_iota(jnp.int32, (S, cols), 0)

        def one(q, carry):
            pick = jnp.where(slot == q * B + b, 1.0, 0.0).astype(jnp.bfloat16)
            idwide[q] = jnp.dot(ids, pick, preferred_element_type=jnp.float32)
            return carry

        lax.fori_loop(0, Q, one, 0)

    def reduce(q):
        def some(step, carry):
            cs = [step * PAIR + u for u in range(PAIR)]
            wants = [c.astype(jnp.float32) for c in cs]
            totals = [None] * PAIR
            for d in range(B):
                name = jnp.broadcast_to(idwide[q, pl.ds(d, 1)], (8, cols))
                value = yrecv[q, d]
                for u in range(PAIR):
                    part = jnp.where((name == wants[u])[None], value, 0.0)
                    totals[u] = part if totals[u] is None else totals[u] + part
            for u in range(PAIR):
                total = totals[u].reshape(freqs, rows, cols)
                out[:, cs[u]] = jnp.where(q > 0, out[:, cs[u]], 0.0) + total
            return carry

        lax.fori_loop(0, chi // PAIR, some, 0)

    def step(s, carry):
        @pl.when(s < Q)
        def _():
            @pl.when(s >= NB)
            def _():
                x_all(s - NB).wait_send()

            @pl.when(s == 0)
            def _():
                compute(s, 0, n // 2)
                pl.semaphore_wait(barrier, T - 1 + B - 1)
                for d in range(1, T):
                    x_copy(s, d, 0, n // 2).start()
                compute(s, n // 2, n)
                for d in range(1, T):
                    x_copy(s, d, n // 2, n - n // 2).start()
                for d in range(1, B):
                    id_copy(d).start()

            @pl.when(s > 0)
            def _():
                compute(s, 0, n)
                for d in range(1, T):
                    x_copy(s, d, 0, n).start()

        @pl.when(s == LX)
        def _():
            idrecv[0] = idrow[...]
            for d in range(1, B):
                id_copy(d).wait()
            widen()

        @pl.when(jnp.logical_and(s >= LX, s < Q + LX))
        def _():
            q = s - LX
            x_all(q).wait_recv()
            transform(q)

            @pl.when(q >= NB)
            def _():
                y_all(q - NB).wait_send()

            pack(q)

        @pl.when(s >= LX + LY)
        def _():
            q = s - LX - LY
            y_all(q).wait_recv()
            reduce(q)

        return carry

    lax.fori_loop(0, Q + LX + LY, step, 0)
    for i in range(min(NB, Q)):
        x_all(Q - 1 - i).wait_send()
        y_all(Q - 1 - i).wait_send()


def pair_of(size, small):
    return (size // small, small)


def body(occupied, virtual, cos_weights, pair_occ, pair_virt, partial_target_tile):
    B = lax.axis_size("tile")
    T = lax.axis_size("tau")
    parts, terms = pair_occ.shape
    freqs = cos_weights.shape[0]
    slots, size = occupied.shape[1:3]
    rows = size // T
    Q = chunks_of(2 * parts // B)
    NB, LX, LY = min(6, Q), 2, 3
    n, blocks = parts // Q, freqs * rows // 8
    f32 = jnp.float32
    smem = pl.BlockSpec(memory_space=pltpu.SMEM)
    vmem = pl.BlockSpec(memory_space=pltpu.VMEM)
    hbm = pl.BlockSpec(memory_space=pltpu.HBM)
    dma = pltpu.SemaphoreType.DMA
    full = -(-parts // 128) * 128
    wide = max(full, Q * B)
    return pl.pallas_call(
        functools.partial(kernel, (pair_of(T, 2), pair_of(B, math.isqrt(B)), Q, NB, LX, LY)),
        out_shape=jax.ShapeDtypeStruct((freqs, CHI_DEV, rows, size), f32),
        in_specs=[hbm, hbm, smem, hbm, hbm, hbm],
        out_specs=vmem,
        scratch_shapes=[
            pltpu.SMEM((terms, parts), jnp.int32),
            pltpu.SMEM((terms, parts), jnp.int32),
            pltpu.VMEM((1, parts), jnp.int32),
            pltpu.VMEM((slots, size, size), occupied.dtype),
            pltpu.VMEM((slots, size, size), virtual.dtype),
            pltpu.VMEM((NB, T, n, rows, size), f32),
            pltpu.VMEM((Q, T - 1, n, rows, size), f32),
            pltpu.VMEM((n, blocks, 8, size), f32),
            pltpu.VMEM((NB, B - 1, blocks, 8, size), f32),
            pltpu.VMEM((Q, B, blocks, 8, size), f32),
            pltpu.VMEM((1, full), jnp.int32),
            pltpu.VMEM((8, wide), jnp.int32),
            pltpu.SMEM((8, wide), jnp.int32),
            pltpu.VMEM((1, Q * B), f32),
            pltpu.VMEM((B, 1, Q * B), f32),
            pltpu.VMEM((Q, B, size), f32),
            dma((NB,)),
            dma((Q,)),
            dma((NB,)),
            dma((Q,)),
            dma((B,)),
            dma((B,)),
            dma((6,)),
        ],
        compiler_params=pltpu.CompilerParams(
            collective_id=0, has_side_effects=True, vmem_limit_bytes=52 * 1024 * 1024
        ),
        name="products",
    )(
        pltpu.with_memory_space_constraint(pair_occ.T, pltpu.HBM),
        pltpu.with_memory_space_constraint(pair_virt.T, pltpu.HBM),
        pltpu.with_memory_space_constraint(cos_weights, pltpu.HBM),
        pltpu.with_memory_space_constraint(partial_target_tile.reshape(1, parts), pltpu.HBM),
        occupied.reshape(slots, size, size),
        virtual.reshape(slots, size, size),
    )


def solution(mesh):
    in_specs = (
        P("tau", "tile", None, None),
        P("tau", "tile", None, None),
        P(),
        P("tile", None),
        P("tile", None),
        P("tile"),
    )
    out_specs = P(None, "tile", "tau", None)
    return jax.shard_map(body, mesh=mesh, in_specs=in_specs, out_specs=out_specs, check_vma=False)
```

```python
import functools
import math

import jax
import jax.numpy as jnp
from jax import lax
from jax.experimental import pallas as pl
from jax.experimental.pallas import tpu as pltpu
from jax.sharding import PartitionSpec as P

CHI_DEV = 32
UNROLL = 2
PAIR = 2
MESH = pl.DeviceIdType.MESH


def chunks_of(cap):
    return 24 if cap % 24 == 0 else cap


def tables(target_ref, padded, table, idrow, Q, owners, chi_dev):
    i32 = jnp.int32
    N, M = target_ref.shape[1], padded.shape[1]
    S = Q * owners
    padded[...] = jnp.full(padded.shape, owners * chi_dev, i32)
    padded[:, pl.ds(0, N)] = target_ref[...]
    target = padded[...]
    up = lax.broadcasted_iota(i32, (M, M), 0)
    across = lax.broadcasted_iota(i32, (M, M), 1)

    def column(row):
        return jnp.transpose(jnp.broadcast_to(row, (8, M)))[:, 0:1]

    def total(chosen, value):
        return jnp.sum(jnp.where(chosen, value, 0), axis=0, keepdims=True)

    key = (target // chi_dev) * M + lax.broadcasted_iota(i32, (1, M), 1)
    target_col = column(target)
    own_col, local_col = target_col // chi_dev, target_col % chi_dev
    key_col = own_col * M + lax.broadcasted_iota(i32, (M, 1), 0)
    place_col = column(total(key_col < key, jnp.ones((M, M), i32)))
    order = total(place_col == across, up)
    slot = lax.broadcasted_iota(i32, (1, S), 1)
    name = slot % owners
    chunk = slot // owners
    one = jnp.ones((M, S), i32)
    first = total(own_col < name, one)
    last = total(own_col <= name, one)
    offset = chunk - first % Q
    place = first + jnp.where(offset < 0, offset + Q, offset)
    found = total(place_col == place, jnp.broadcast_to(local_col, (M, S)))
    idrow[...] = jnp.where(place < last, found, -1).astype(jnp.float32)
    table[pl.ds(0, 1), pl.ds(0, M)] = jnp.minimum(order, N - 1)
    table[pl.ds(1, 1), pl.ds(0, S)] = jnp.minimum(place // Q, N // Q - 1)


def around(me, offset, sizes):
    (a, b), (big, small) = offset, sizes
    return lax.rem(me // small + a, big) * small + lax.rem(me + b, small)


def offsets(sizes):
    every = [(a, b) for a in range(sizes[0]) for b in range(sizes[1])]
    far = lambda v, n: min(v, n - v)
    return every[:1] + sorted(every[1:], reverse=True, key=lambda o: (far(o[0], sizes[0]) + far(o[1], sizes[1]), o[0] * o[1] > 0, o[0] + o[1], o))


def back(offset, sizes):
    return tuple((n - v) % n for v, n in zip(offset, sizes))


def kernel(
    cfg, pair_occ_hbm, pair_virt_hbm, weights, target_hbm, occ_hbm, virt_hbm, out,
    pair_occ, pair_virt, target, occ, virt, stage, xrecv, spec, ysend, yrecv, padded, table, smem, idrow, idrecv, idwide,
    xs, xr, ys, yr, ids_s, ids_r, load,
):
    tau, tile, Q, NB, LX, LY = cfg
    T, B = tau[0] * tau[1], tile[0] * tile[1]
    terms = pair_occ.shape[0]
    n = stage.shape[2]
    rows, cols = stage.shape[3:]
    freqs, chi = out.shape[:2]
    t = lax.axis_index("tau")
    b = lax.axis_index("tile")
    near_t, near_b = offsets(tau), offsets(tile)
    half = B // 2

    def tau_at(d):
        return around(t, near_t[d], tau)

    def tile_at(d):
        return around(b, near_b[d], tile)

    names = pltpu.make_async_copy(target_hbm, target, load.at[3])
    names.start()
    loads = [
        pltpu.make_async_copy(pair_occ_hbm, pair_occ, load.at[4]),
        pltpu.make_async_copy(pair_virt_hbm, pair_virt, load.at[5]),
        pltpu.make_async_copy(occ_hbm, occ, load.at[0]),
        pltpu.make_async_copy(virt_hbm, virt, load.at[1]),
    ]
    for copy in loads:
        copy.start()
    barrier = pltpu.get_barrier_semaphore()
    for d in range(1, T):
        pl.semaphore_signal(barrier, inc=1, device_id=(tau_at(d), b), device_id_type=MESH)
    for d in range(1, B):
        pl.semaphore_signal(barrier, inc=1, device_id=(t, tile_at(d)), device_id_type=MESH)
    names.wait()
    tables(target, padded, table, idrow, Q, B, chi)
    down = pltpu.make_async_copy(table, smem, load.at[2])
    down.start()
    down.wait()
    for copy in loads:
        copy.wait()

    def compute(s, lo, hi):
        buf = lax.rem(s, NB)

        def some(step, carry):
            for u in range(UNROLL):
                i = step * UNROLL + u
                p = smem[0, s + Q * i]
                left = jnp.concatenate([occ[pair_occ[j, p]] for j in range(terms)], axis=1)
                right = jnp.concatenate([virt[pair_virt[j, p]] for j in range(terms)], axis=0)
                product = jnp.dot(left, right, preferred_element_type=jnp.float32)
                for g in range(T):
                    stage[buf, g, i] = product[g * rows : (g + 1) * rows]
            return carry

        lax.fori_loop(lo // UNROLL, hi // UNROLL, some, 0)

    def x_copy(s, d, lo, size):
        buf = lax.rem(s, NB)
        to = tau_at(d)
        return pltpu.make_async_remote_copy(
            src_ref=stage.at[buf, to, pl.ds(lo, size)],
            dst_ref=xrecv.at[s, d - 1, pl.ds(lo, size)],
            send_sem=xs.at[buf],
            recv_sem=xr.at[s],
            device_id=(to, b),
            device_id_type=MESH,
        )

    def x_all(s):
        return pltpu.make_async_remote_copy(
            src_ref=stage.at[lax.rem(s, NB), pl.ds(0, T - 1)],
            dst_ref=xrecv.at[s],
            send_sem=xs.at[lax.rem(s, NB)],
            recv_sem=xr.at[s],
            device_id=(tau_at(1), b),
            device_id_type=MESH,
        )

    def y_copy(q, d):
        buf = lax.rem(q, NB)
        return pltpu.make_async_remote_copy(
            src_ref=ysend.at[buf, d - 1],
            dst_ref=yrecv.at[q, d],
            send_sem=ys.at[buf],
            recv_sem=yr.at[q, int(d >= half)],
            device_id=(t, tile_at(d)),
            device_id_type=MESH,
        )

    def y_all(q):
        return pltpu.make_async_remote_copy(
            src_ref=ysend.at[lax.rem(q, NB)],
            dst_ref=yrecv.at[q, pl.ds(1, B - 1)],
            send_sem=ys.at[lax.rem(q, NB)],
            recv_sem=yr.at[q, 0],
            device_id=(t, tile_at(1)),
            device_id_type=MESH,
        )

    def y_part(q, lo, hi):
        return pltpu.make_async_remote_copy(
            src_ref=ysend.at[lax.rem(q, NB), pl.ds(lo - 1, hi - lo)],
            dst_ref=yrecv.at[q, pl.ds(lo, hi - lo)],
            send_sem=ys.at[lax.rem(q, NB)],
            recv_sem=yr.at[q, int(lo >= half)],
            device_id=(t, tile_at(1)),
            device_id_type=MESH,
        )

    def id_copy(d):
        return pltpu.make_async_remote_copy(
            src_ref=idrow,
            dst_ref=idrecv.at[d],
            send_sem=ids_s.at[d],
            recv_sem=ids_r.at[d],
            device_id=(t, tile_at(d)),
            device_id_type=MESH,
        )

    def transform(q):
        buf = lax.rem(q, NB)
        w = [[weights[k, around(t, back(near_t[d], tau), tau)] for k in range(freqs)] for d in range(T)]

        def one(i, carry):
            total = [None] * freqs
            for d in range(T):
                v = stage[buf, t, i] if d == 0 else xrecv[q, d - 1, i]
                for k in range(freqs):
                    term = v * w[d][k]
                    total[k] = term if total[k] is None else total[k] + term
            for k in range(freqs):
                for r in range(rows // 8):
                    spec[i, k * (rows // 8) + r] = total[k][r * 8 : r * 8 + 8]
            return carry

        lax.fori_loop(0, n, one, 0)

    def pack(q):
        buf = lax.rem(q, NB)
        yrecv[q, 0] = spec[smem[1, q * B + b]]
        for d in range(1, B):
            ysend[buf, d - 1] = spec[smem[1, q * B + tile_at(d)]]
            y_copy(q, d).start()

    def widen():
        S = Q * B
        ids = jnp.concatenate([idrecv[d] for d in range(B)], axis=0).astype(jnp.bfloat16)
        slot = lax.broadcasted_iota(jnp.int32, (S, cols), 0)

        def one(q, carry):
            pick = jnp.where(slot == q * B + b, 1.0, 0.0).astype(jnp.bfloat16)
            idwide[q] = jnp.dot(ids, pick, preferred_element_type=jnp.float32)
            return carry

        lax.fori_loop(0, Q, one, 0)

    def reduce(q, lo, hi):
        def some(step, carry):
            cs = [step * PAIR + u for u in range(PAIR)]
            wants = [c.astype(jnp.float32) for c in cs]
            totals = [None] * PAIR
            for d in range(lo, hi):
                name = jnp.broadcast_to(idwide[q, pl.ds(d, 1)], (8, cols))
                value = yrecv[q, d]
                for u in range(PAIR):
                    part = jnp.where((name == wants[u])[None], value, 0.0)
                    totals[u] = part if totals[u] is None else totals[u] + part
            for u in range(PAIR):
                total = totals[u].reshape(freqs, rows, cols)
                kept = out[:, cs[u]]
                if lo == 0:
                    kept = jnp.where(q > 0, kept, 0.0)
                out[:, cs[u]] = kept + total
            return carry

        lax.fori_loop(0, chi // PAIR, some, 0)

    def step(s, carry):
        @pl.when(s < Q)
        def _():
            @pl.when(s >= NB)
            def _():
                x_all(s - NB).wait_send()

            @pl.when(s == 0)
            def _():
                compute(s, 0, n // 2)
                pl.semaphore_wait(barrier, T - 1 + B - 1)
                for d in range(1, T):
                    x_copy(s, d, 0, n // 2).start()
                compute(s, n // 2, n)
                for d in range(1, T):
                    x_copy(s, d, n // 2, n - n // 2).start()
                for d in range(1, B):
                    id_copy(d).start()

            @pl.when(s > 0)
            def _():
                compute(s, 0, n)
                for d in range(1, T):
                    x_copy(s, d, 0, n).start()

        @pl.when(s == LX)
        def _():
            idrecv[0] = idrow[...]
            for d in range(1, B):
                id_copy(d).wait()
            widen()

        @pl.when(jnp.logical_and(s >= LX, s < Q + LX))
        def _():
            q = s - LX
            x_all(q).wait_recv()
            transform(q)

            @pl.when(q >= NB)
            def _():
                y_all(q - NB).wait_send()

            pack(q)

        @pl.when(s >= LX + LY)
        def _():
            q = s - LX - LY
            y_part(q, 1, half).wait_recv()
            reduce(q, 0, half)
            y_part(q, half, B).wait_recv()
            reduce(q, half, B)

        return carry

    lax.fori_loop(0, Q + LX + LY, step, 0)
    for i in range(min(NB, Q)):
        x_all(Q - 1 - i).wait_send()
        y_all(Q - 1 - i).wait_send()


def pair_of(size, small):
    return (size // small, small)


def body(occupied, virtual, cos_weights, pair_occ, pair_virt, partial_target_tile):
    B = lax.axis_size("tile")
    T = lax.axis_size("tau")
    parts, terms = pair_occ.shape
    freqs = cos_weights.shape[0]
    slots, size = occupied.shape[1:3]
    rows = size // T
    Q = chunks_of(2 * parts // B)
    NB, LX, LY = min(6, Q), 2, 3
    n, blocks = parts // Q, freqs * rows // 8
    f32 = jnp.float32
    smem = pl.BlockSpec(memory_space=pltpu.SMEM)
    vmem = pl.BlockSpec(memory_space=pltpu.VMEM)
    hbm = pl.BlockSpec(memory_space=pltpu.HBM)
    dma = pltpu.SemaphoreType.DMA
    full = -(-parts // 128) * 128
    wide = max(full, Q * B)
    return pl.pallas_call(
        functools.partial(kernel, (pair_of(T, 2), pair_of(B, math.isqrt(B)), Q, NB, LX, LY)),
        out_shape=jax.ShapeDtypeStruct((freqs, CHI_DEV, rows, size), f32),
        in_specs=[hbm, hbm, smem, hbm, hbm, hbm],
        out_specs=vmem,
        scratch_shapes=[
            pltpu.SMEM((terms, parts), jnp.int32),
            pltpu.SMEM((terms, parts), jnp.int32),
            pltpu.VMEM((1, parts), jnp.int32),
            pltpu.VMEM((slots, size, size), occupied.dtype),
            pltpu.VMEM((slots, size, size), virtual.dtype),
            pltpu.VMEM((NB, T, n, rows, size), f32),
            pltpu.VMEM((Q, T - 1, n, rows, size), f32),
            pltpu.VMEM((n, blocks, 8, size), f32),
            pltpu.VMEM((NB, B - 1, blocks, 8, size), f32),
            pltpu.VMEM((Q, B, blocks, 8, size), f32),
            pltpu.VMEM((1, full), jnp.int32),
            pltpu.VMEM((8, wide), jnp.int32),
            pltpu.SMEM((8, wide), jnp.int32),
            pltpu.VMEM((1, Q * B), f32),
            pltpu.VMEM((B, 1, Q * B), f32),
            pltpu.VMEM((Q, B, size), f32),
            dma((NB,)),
            dma((Q,)),
            dma((NB,)),
            dma((Q, 2)),
            dma((B,)),
            dma((B,)),
            dma((6,)),
        ],
        compiler_params=pltpu.CompilerParams(
            collective_id=0, has_side_effects=True, vmem_limit_bytes=52 * 1024 * 1024
        ),
        name="products",
    )(
        pltpu.with_memory_space_constraint(pair_occ.T, pltpu.HBM),
        pltpu.with_memory_space_constraint(pair_virt.T, pltpu.HBM),
        pltpu.with_memory_space_constraint(cos_weights, pltpu.HBM),
        pltpu.with_memory_space_constraint(partial_target_tile.reshape(1, parts), pltpu.HBM),
        occupied.reshape(slots, size, size),
        virtual.reshape(slots, size, size),
    )


def solution(mesh):
    in_specs = (
        P("tau", "tile", None, None),
        P("tau", "tile", None, None),
        P(),
        P("tile", None),
        P("tile", None),
        P("tile"),
    )
    out_specs = P(None, "tile", "tau", None)
    return jax.shard_map(body, mesh=mesh, in_specs=in_specs, out_specs=out_specs, check_vma=False)
```
